128 devices in a mesh: ens: 1, col: 16 (over z, y), row: 8 (over x, core).
Axes of the slice: x: 4, y: 4, z: 4, core: 2. Of those that a mesh axis runs over, the one named last changes fastest.
Arguments:
- images: bfloat16 [32, 64, 512, 256], P('ens', 'row', 'col')
- w_conv: bfloat16 [4, 3, 3, 256, 256], replicated
- b_conv: float32 [4, 256], replicated
Outputs:
- output: bfloat16 [32, 64, 512, 256], P('ens', 'row', 'col')
All inputs are finite; a program needn't handle non-finite values.
Results may differ from the reference program's by a relative error of at most 0.00389.
Values are sent between devices in bfloat16 or wider.
A program may use at most 1 GiB of HBM per device.

```python
import jax
import jax.numpy as jnp
from jax import lax

CH = 256
BATCH = 32
TILE_H = 8
TILE_W = 32
ROW_DEVS = 8
COL_DEVS = 16
LAYERS = 4
HEIGHT = TILE_H * ROW_DEVS
WIDTH = TILE_W * COL_DEVS
CONV_DIMS = ("NHWC", "HWIO", "NHWC")


def setup_inputs(seed: int = 0, part: int = 0) -> dict:
    base_key = jax.random.key(seed)
    image_key = jax.random.fold_in(jax.random.fold_in(base_key, 1), part)
    weight_key, bias_key = jax.random.split(jax.random.fold_in(base_key, 2))
    images = jax.random.normal(image_key, (BATCH, HEIGHT, WIDTH, CH), jnp.float32)
    w_scale = (2.0 / (9 * CH)) ** 0.5
    w_conv = jax.random.normal(weight_key, (LAYERS, 3, 3, CH, CH), jnp.float32) * w_scale
    b_conv = 0.3 * jax.random.normal(bias_key, (LAYERS, CH), jnp.float32)
    return {"images": images.astype(jnp.bfloat16), "w_conv": w_conv.astype(jnp.bfloat16), "b_conv": b_conv}


def reference(images, w_conv, b_conv):
    def one_image(image):
        def layer_step(hidden_in, layer_params):
            w_layer, b_layer = layer_params
            summed = lax.conv_general_dilated(hidden_in.astype(jnp.float32), w_layer.astype(jnp.float32), (1, 1), ((1, 1), (1, 1)), dimension_numbers=CONV_DIMS, precision=lax.Precision.HIGHEST)
            return jnp.maximum(summed + b_layer, 0.0).astype(jnp.bfloat16), None
        final_state = lax.scan(layer_step, image[None], (w_conv, b_conv))[0]
        return final_state[0]
    return lax.map(one_image, images)
```

```python
import functools

import jax
import jax.numpy as jnp
from jax import lax
from jax.experimental import pallas as pl
from jax.experimental.pallas import tpu as pltpu
from jax.sharding import PartitionSpec as P

MESH = pl.DeviceIdType.MESH
LANES = 128
GROUPS = 2
ROW_ORDER = (0, 7, 1, 2, 3, 4, 5, 6)


def kernel(dims, x_hbm, w_hbm, b_ref, o_hbm, act, w_vm, in_sem, out_sem, send_sem, recv_sem):
    layers, imgs, rows, cols, ch, row_devs, col_devs = dims
    halves = ch // LANES
    taps = 9
    row, col = lax.axis_index("row"), lax.axis_index("col")
    has = {(-1, 0): row > 0, (1, 0): row < row_devs - 1, (0, -1): col > 0, (0, 1): col < col_devs - 1}

    def exists(dr, dc):
        if dr and dc:
            return jnp.logical_and(has[(dr, 0)], has[(0, dc)])
        return has[(dr, dc)]

    def span(step, size):
        if step < 0:
            return pl.ds(1, 1), pl.ds(size + 1, 1)
        if step > 0:
            return pl.ds(size, 1), pl.ds(0, 1)
        return pl.ds(1, size), pl.ds(1, size)

    nbrs = [(-1, 0), (1, 0), (0, -1), (0, 1), (-1, -1), (-1, 1), (1, -1), (1, 1)]

    def edge_copy(buf, n):
        dr, dc = nbrs[n]
        src_r, dst_r = span(dr, rows)
        src_c, dst_c = span(dc, cols)
        return pltpu.make_async_remote_copy(
            src_ref=act.at[buf, src_r, src_c],
            dst_ref=act.at[buf, dst_r, dst_c],
            send_sem=send_sem.at[buf, n],
            recv_sem=recv_sem.at[buf, n],
            device_id={"row": row + dr, "col": col + dc},
            device_id_type=MESH,
        )

    def send(buf, which):
        for n in which:
            @pl.when(exists(*nbrs[n]))
            def _(n=n):
                edge_copy(buf, n).start()

    w_copies = []
    for l in range(layers):
        for hf in range(halves):
            w_copies.append(pltpu.make_async_copy(
                w_hbm.at[l, :, pl.ds(hf * LANES, LANES)],
                w_vm.at[l, hf], in_sem.at[GROUPS + l * halves + hf]))
    x_copies = [pltpu.make_async_copy(x_hbm.at[g], act.at[g, pl.ds(1, rows), pl.ds(1, cols)], in_sem.at[g]) for g in range(GROUPS)]
    for c in x_copies:
        c.start()
    for c in w_copies:
        c.start()

    barrier = pltpu.get_barrier_semaphore()
    for n, (dr, dc) in enumerate(nbrs):
        @pl.when(exists(dr, dc))
        def _(dr=dr, dc=dc):
            pl.semaphore_signal(barrier, inc=1, device_id={"row": row + dr, "col": col + dc}, device_id_type=MESH)
    n_row = 1 + sum(has[(d, 0)].astype(jnp.int32) for d in (-1, 1))
    n_col = 1 + sum(has[(0, d)].astype(jnp.int32) for d in (-1, 1))
    pl.semaphore_wait(barrier, n_row * n_col - 1)

    for g in range(GROUPS):
        x_copies[g].wait()
        send(g, range(8))

    def zero_borders(buf, carry):
        @pl.when(row == 0)
        def _():
            act[buf, 0] = jnp.zeros(act.shape[2:], act.dtype)

        @pl.when(row == row_devs - 1)
        def _():
            act[buf, rows + 1] = jnp.zeros(act.shape[2:], act.dtype)

        @pl.when(col == 0)
        def _():
            act[buf, :, 0] = jnp.zeros((rows + 2,) + act.shape[3:], act.dtype)

        @pl.when(col == col_devs - 1)
        def _():
            act[buf, :, cols + 1] = jnp.zeros((rows + 2,) + act.shape[3:], act.dtype)
        return carry

    lax.fori_loop(0, layers * GROUPS, zero_borders, 0)
    for c in w_copies:
        c.wait()

    def row_out(p, buf, layer, r):
        pieces = []
        for t in range(taps):
            tap = act[p, r + t // 3, pl.ds(t % 3, cols)]
            pieces += [tap[:, hf].reshape(cols * imgs, LANES) for hf in range(halves)]
        lhs = jnp.concatenate(pieces, axis=1)
        wt = jnp.concatenate([w_vm[layer, hf] for hf in range(halves)], axis=1)
        y = jnp.dot(lhs, wt, preferred_element_type=jnp.float32)
        y = jnp.maximum(y + b_ref[layer], 0.0).astype(jnp.bfloat16)
        for hf in range(halves):
            act[buf, r + 1, pl.ds(1, cols), hf] = y[:, hf * LANES:(hf + 1) * LANES].reshape(cols, imgs, LANES)

    def phase(p, carry):
        layer = p // GROUPS
        for n in range(8):
            @pl.when(exists(-nbrs[n][0], -nbrs[n][1]))
            def _(n=n):
                edge_copy(p, n).wait_recv()

        for i, r in enumerate(ROW_ORDER):
            row_out(p, p + GROUPS, layer, r)
            if i == 3:
                @pl.when(p < (layers - 1) * GROUPS)
                def _():
                    send(p + GROUPS, (0, 1, 4, 5, 6, 7))
        @pl.when(p < (layers - 1) * GROUPS)
        def _():
            send(p + GROUPS, (2, 3))
        return carry

    lax.fori_loop(0, layers * GROUPS, phase, 0)

    out_copies = [pltpu.make_async_copy(act.at[layers * GROUPS + g, pl.ds(1, rows), pl.ds(1, cols)], o_hbm.at[g], out_sem.at[g]) for g in range(GROUPS)]
    for c in out_copies:
        c.start()

    def finish(buf, carry):
        for n in range(8):
            @pl.when(exists(*nbrs[n]))
            def _(n=n):
                edge_copy(buf, n).wait_send()
        return carry

    lax.fori_loop(0, layers * GROUPS, finish, 0)
    for c in out_copies:
        c.wait()


def solution(mesh):
    row_devs = mesh.shape["row"]
    col_devs = mesh.shape["col"]
    act_spec = P("ens", "row", "col", None)

    def local_stack(x_tile, weights, biases):
        batch, rows, cols, ch = x_tile.shape
        layers = weights.shape[0]
        imgs = batch // GROUPS
        halves = ch // LANES
        dims = (layers, imgs, rows, cols, ch, row_devs, col_devs)
        x = x_tile.reshape(GROUPS, imgs, rows, cols, halves, LANES).transpose(0, 2, 3, 4, 1, 5)
        w = weights.reshape(layers, 9 * ch, ch)
        b = biases.reshape(layers, 1, ch)
        any_spec = pl.BlockSpec(memory_space=pl.ANY)
        y = pl.pallas_call(
            functools.partial(kernel, dims),
            out_shape=jax.ShapeDtypeStruct((GROUPS, rows, cols, halves, imgs, LANES), jnp.bfloat16),
            in_specs=[any_spec, any_spec, pl.BlockSpec(memory_space=pltpu.VMEM)],
            out_specs=any_spec,
            scratch_shapes=[
                pltpu.VMEM(((layers + 1) * GROUPS, rows + 2, cols + 2, halves, imgs, LANES), jnp.bfloat16),
                pltpu.VMEM((layers, halves, 9 * ch, LANES), jnp.bfloat16),
                pltpu.SemaphoreType.DMA((GROUPS + layers * halves,)),
                pltpu.SemaphoreType.DMA((GROUPS,)),
                pltpu.SemaphoreType.DMA((layers * GROUPS, 8)),
                pltpu.SemaphoreType.DMA((layers * GROUPS, 8)),
            ],
            compiler_params=pltpu.CompilerParams(collective_id=0, has_side_effects=True, vmem_limit_bytes=48 * 1024 * 1024),
            name="conv_stack",
        )(x, w, b)
        return y.transpose(0, 4, 1, 2, 3, 5).reshape(batch, rows, cols, ch)

    return jax.shard_map(local_stack, mesh=mesh, in_specs=(act_spec, P(), P()), out_specs=act_spec, check_vma=False)
```

```python
import functools

import jax
import jax.numpy as jnp
from jax import lax
from jax.experimental import pallas as pl
from jax.experimental.pallas import tpu as pltpu
from jax.sharding import PartitionSpec as P

MESH = pl.DeviceIdType.MESH
LANES = 128
GROUPS = 2
TAPS = 9
NBRS = ((-1, 0), (1, 0), (0, -1), (0, 1), (-1, -1), (-1, 1), (1, -1), (1, 1))
ROW_SENDS = (0, 1, 4, 5, 6, 7)
COL_SENDS = (2, 3)


def kernel(dims, x_hbm, w_hbm, b_hbm, o_ref, act, w_vm, b_ref, x_vm, perm, turn, in_sem, send_sem, recv_sem):
    layers, imgs, rows, cols, ch, row_devs, col_devs = dims
    halves = ch // LANES
    pitch = cols + 8
    row, col = lax.axis_index("row"), lax.axis_index("col")
    has = {(-1, 0): row > 0, (1, 0): row < row_devs - 1, (0, -1): col > 0, (0, 1): col < col_devs - 1}

    def exists(dr, dc):
        if dr and dc:
            return jnp.logical_and(has[(dr, 0)], has[(0, dc)])
        return has[(dr, dc)]

    def span(step, size):
        if step < 0:
            return pl.ds(1, 1), pl.ds(size + 1, 1)
        if step > 0:
            return pl.ds(size, 1), pl.ds(0, 1)
        return pl.ds(1, size), pl.ds(1, size)

    def edge_copy(buf, n):
        dr, dc = NBRS[n]
        src_r, dst_r = span(dr, rows)
        src_c, dst_c = span(dc, cols)
        return pltpu.make_async_remote_copy(
            src_ref=act.at[buf, src_r, src_c],
            dst_ref=act.at[buf, dst_r, dst_c],
            send_sem=send_sem.at[buf, n],
            recv_sem=recv_sem.at[buf, n],
            device_id={"row": row + dr, "col": col + dc},
            device_id_type=MESH,
        )

    def send(buf, which):
        for n in which:
            @pl.when(exists(*NBRS[n]))
            def _(n=n):
                edge_copy(buf, n).start()

    def receive(buf):
        for n, (dr, dc) in enumerate(NBRS):
            @pl.when(exists(-dr, -dc))
            def _(n=n):
                edge_copy(buf, n).wait_recv()

    x_copies, w_copies = [], []
    for g in range(GROUPS):
        for hf in range(halves):
            x_copies.append(pltpu.make_async_copy(
                x_hbm.at[pl.ds(g * imgs, imgs), :, :, pl.ds(hf * LANES, LANES)], x_vm.at[g, hf], in_sem.at[g * halves + hf]))
    for l in range(layers):
        for hf in range(halves):
            w_copies.append(pltpu.make_async_copy(
                w_hbm.at[l, :, pl.ds(hf * LANES, LANES)], w_vm.at[l, hf], in_sem.at[(GROUPS + l) * halves + hf]))
    b_copy = pltpu.make_async_copy(b_hbm, b_ref, in_sem.at[(GROUPS + layers) * halves])
    for c in x_copies + w_copies + [b_copy]:
        c.start()

    barrier = pltpu.get_barrier_semaphore()
    for dr, dc in NBRS:
        @pl.when(exists(dr, dc))
        def _(dr=dr, dc=dc):
            pl.semaphore_signal(barrier, inc=1, device_id={"row": row + dr, "col": col + dc}, device_id_type=MESH)

    def zero_borders(buf, carry):
        @pl.when(row == 0)
        def _():
            act[buf, 0] = jnp.zeros(act.shape[2:], act.dtype)

        @pl.when(row == row_devs - 1)
        def _():
            act[buf, rows + 1] = jnp.zeros(act.shape[2:], act.dtype)

        @pl.when(col == 0)
        def _():
            act[buf, :, 0] = jnp.zeros((rows + 2,) + act.shape[3:], act.dtype)

        @pl.when(col == col_devs - 1)
        def _():
            act[buf, :, cols + 1] = jnp.zeros((rows + 2,) + act.shape[3:], act.dtype)
        return carry

    lax.fori_loop(0, layers * GROUPS, zero_borders, 0)

    block = imgs * imgs
    out_row = lax.broadcasted_iota(jnp.int32, (block, block), 0)
    in_row = lax.broadcasted_iota(jnp.int32, (block, block), 1)
    swapped = (out_row % imgs) * imgs + out_row // imgs
    perm[...] = jnp.where(in_row == swapped, 1.0, 0.0).astype(jnp.bfloat16)

    n_row = 1 + sum(has[(d, 0)].astype(jnp.int32) for d in (-1, 1))
    n_col = 1 + sum(has[(0, d)].astype(jnp.int32) for d in (-1, 1))
    pl.semaphore_wait(barrier, n_row * n_col - 1)

    def put(buf, r, first, count, y):
        for hf in range(halves):
            act[buf, r + 1, pl.ds(first + 1, count), hf] = y[:, hf * LANES:(hf + 1) * LANES].reshape(count, imgs, LANES)

    order = (0, rows - 1) + tuple(range(1, rows - 1))
    for g in range(GROUPS):
        for hf in range(halves):
            x_copies[g * halves + hf].wait()
        for i, r in enumerate(order):
            for first in range(0, cols, imgs):
                tile = jnp.concatenate([x_vm[g, hf, :, r, pl.ds(first, imgs)].reshape(block, LANES) for hf in range(halves)], axis=1)
                y = jnp.dot(perm[...], tile, preferred_element_type=jnp.float32)
                put(g, r, first, imgs, y.astype(jnp.bfloat16))
            if i == 2:
                send(g, ROW_SENDS)
        send(g, COL_SENDS)
    for c in w_copies + [b_copy]:
        c.wait()

    def conv(taps, layer):
        lhs = jnp.concatenate([tap[..., hf, :, :].reshape(-1, LANES) for tap in taps for hf in range(halves)], axis=1)
        wt = jnp.concatenate([w_vm[layer, hf] for hf in range(halves)], axis=1)
        y = jnp.dot(lhs, wt, preferred_element_type=jnp.float32)
        return jnp.maximum(y + b_ref[pl.ds(layer, 1), :], 0.0)

    def conv_row(p, layer, r, first, count):
        return conv([act[p, r + t // 3, pl.ds(first + t % 3, count)] for t in range(TAPS)], layer)

    def first_layer(g, carry):
        for r in range(1, rows - 1):
            y = conv_row(g, 0, r, 1, cols - 2)
            put(g + GROUPS, r, 1, cols - 2, y.astype(jnp.bfloat16))
        receive(g)
        for r in (0, rows - 1):
            y = conv_row(g, 0, r, 0, cols)
            put(g + GROUPS, r, 0, cols, y.astype(jnp.bfloat16))
        taps = []
        for t in range(TAPS):
            sides = [act[g, pl.ds(1 + t // 3, rows - 2), c + t % 3] for c in (0, cols - 1)]
            taps.append(jnp.concatenate(sides, axis=0))
        y = conv(taps, 0).astype(jnp.bfloat16)
        half = (rows - 2) * imgs
        for s, c in enumerate((0, cols - 1)):
            for hf in range(halves):
                piece = y[s * half:(s + 1) * half, hf * LANES:(hf + 1) * LANES]
                act[g + GROUPS, pl.ds(2, rows - 2), c + 1, hf] = piece.reshape(rows - 2, imgs, LANES)
        send(g + GROUPS, ROW_SENDS + COL_SENDS)
        return carry

    lax.fori_loop(0, GROUPS, first_layer, 0)

    def middle_layer(p, carry):
        receive(p)
        for i, r in enumerate(order):
            y = conv_row(p, p // GROUPS, r, 0, cols)
            put(p + GROUPS, r, 0, cols, y.astype(jnp.bfloat16))
            if i == 2:
                send(p + GROUPS, ROW_SENDS)
        send(p + GROUPS, COL_SENDS)
        return carry

    lax.fori_loop(GROUPS, (layers - 1) * GROUPS, middle_layer, 0)

    def last_layer(g, carry):
        p = (layers - 1) * GROUPS + g
        receive(p)
        for r in range(rows):
            y = conv_row(p, layers - 1, r, 0, cols)
            for c in range(cols):
                for hf in range(halves):
                    turn[r % 2, hf, pl.ds(c, imgs, stride=pitch), :] = y[c * imgs:(c + 1) * imgs, hf * LANES:(hf + 1) * LANES]
            for i in range(imgs):
                for hf in range(halves):
                    line = turn[r % 2, hf, pl.ds(i * pitch, cols), :].astype(jnp.bfloat16)
                    o_ref[g * imgs + i, r, :, pl.ds(hf * LANES, LANES)] = line
        return carry

    lax.fori_loop(0, GROUPS, last_layer, 0)

    def finish(buf, carry):
        for n in range(len(NBRS)):
            @pl.when(exists(*NBRS[n]))
            def _(n=n):
                edge_copy(buf, n).wait_send()
        return carry

    lax.fori_loop(0, layers * GROUPS, finish, 0)


def solution(mesh):
    row_devs = mesh.shape["row"]
    col_devs = mesh.shape["col"]
    act_spec = P("ens", "row", "col", None)

    def local_stack(x_tile, weights, biases):
        batch, rows, cols, ch = x_tile.shape
        layers = weights.shape[0]
        imgs = batch // GROUPS
        halves = ch // LANES
        dims = (layers, imgs, rows, cols, ch, row_devs, col_devs)
        hbm = pl.BlockSpec(memory_space=pltpu.HBM)
        return pl.pallas_call(
            functools.partial(kernel, dims),
            out_shape=pltpu.VMEM((batch, rows, cols, ch), jnp.bfloat16),
            in_specs=[hbm, hbm, hbm],
            out_specs=pl.BlockSpec(memory_space=pltpu.VMEM),
            scratch_shapes=[
                pltpu.VMEM((layers * GROUPS, rows + 2, cols + 2, halves, imgs, LANES), jnp.bfloat16),
                pltpu.VMEM((layers, halves, TAPS * ch, LANES), jnp.bfloat16),
                pltpu.VMEM((layers, ch), jnp.float32),
                pltpu.VMEM((GROUPS, halves, imgs, rows, cols, LANES), jnp.bfloat16),
                pltpu.VMEM((imgs * imgs, imgs * imgs), jnp.bfloat16),
                pltpu.VMEM((2, halves, imgs * (cols + 8), LANES), jnp.float32),
                pltpu.SemaphoreType.DMA(((GROUPS + layers) * halves + 1,)),
                pltpu.SemaphoreType.DMA((layers * GROUPS, len(NBRS))),
                pltpu.SemaphoreType.DMA((layers * GROUPS, len(NBRS))),
            ],
            compiler_params=pltpu.CompilerParams(collective_id=0, has_side_effects=True, vmem_limit_bytes=56 * 1024 * 1024),
            name="conv_stack",
        )(x_tile, weights.reshape(layers, TAPS * ch, ch), biases)

    return jax.shard_map(local_stack, mesh=mesh, in_specs=(act_spec, P(), P()), out_specs=act_spec, check_vma=False)
```

```python
import functools

import jax
import jax.numpy as jnp
from jax import lax
from jax.experimental import pallas as pl
from jax.experimental.pallas import tpu as pltpu
from jax.sharding import PartitionSpec as P

MESH = pl.DeviceIdType.MESH
LANES = 128
GROUPS = 2
TAPS = 9
NBRS = ((-1, 0), (1, 0), (0, -1), (0, 1), (-1, -1), (-1, 1), (1, -1), (1, 1))
ROW_SENDS = (0, 1, 4, 5, 6, 7)
COL_SENDS = (2, 3)


def kernel(dims, x_hbm, w_hbm, b_hbm, o_ref, act, w_vm, b_ref, x_vm, perm, turn, in_sem, send_sem, recv_sem):
    layers, imgs, rows, cols, ch, row_devs, col_devs = dims
    halves = ch // LANES
    pitch = cols + 8
    row, col = lax.axis_index("row"), lax.axis_index("col")

    def span(step, size, at, devs):
        if step < 0:
            return pl.ds(1, 1), pl.ds(jnp.where(at == 0, size + 2, size + 1), 1), lax.rem(at + devs - 1, devs)
        if step > 0:
            return pl.ds(size, 1), pl.ds(jnp.where(at == devs - 1, size + 2, 0), 1), lax.rem(at + 1, devs)
        return pl.ds(1, size), pl.ds(1, size), at

    spans = {}
    for step in (-1, 0, 1):
        spans["row", step] = span(step, rows, row, row_devs)
        spans["col", step] = span(step, cols, col, col_devs)

    def neighbour(n):
        return {"row": spans["row", NBRS[n][0]][2], "col": spans["col", NBRS[n][1]][2]}

    def edge_copy(buf, n):
        src_r, dst_r, _ = spans["row", NBRS[n][0]]
        src_c, dst_c, _ = spans["col", NBRS[n][1]]
        return pltpu.make_async_remote_copy(
            src_ref=act.at[buf, src_r, src_c],
            dst_ref=act.at[buf, dst_r, dst_c],
            send_sem=send_sem.at[buf, n],
            recv_sem=recv_sem.at[buf, n],
            device_id=neighbour(n),
            device_id_type=MESH,
        )

    def send(buf, which):
        for n in which:
            edge_copy(buf, n).start()

    def receive(buf):
        for n in range(len(NBRS)):
            edge_copy(buf, n).wait_recv()

    x_copies, w_copies = [], []
    for g in range(GROUPS):
        for hf in range(halves):
            x_copies.append(pltpu.make_async_copy(
                x_hbm.at[pl.ds(g * imgs, imgs), :, :, pl.ds(hf * LANES, LANES)], x_vm.at[g, hf], in_sem.at[g * halves + hf]))
    for l in range(layers):
        for hf in range(halves):
            w_copies.append(pltpu.make_async_copy(
                w_hbm.at[l, :, pl.ds(hf * LANES, LANES)], w_vm.at[l, hf], in_sem.at[(GROUPS + l) * halves + hf]))
    b_copy = pltpu.make_async_copy(b_hbm, b_ref, in_sem.at[(GROUPS + layers) * halves])
    for c in x_copies + w_copies + [b_copy]:
        c.start()

    barrier = pltpu.get_barrier_semaphore()
    for n in range(len(NBRS)):
        pl.semaphore_signal(barrier, inc=1, device_id=neighbour(n), device_id_type=MESH)

    def zero_borders(buf, carry):
        @pl.when(row == 0)
        def _():
            act[buf, 0] = jnp.zeros(act.shape[2:], act.dtype)

        @pl.when(row == row_devs - 1)
        def _():
            act[buf, rows + 1] = jnp.zeros(act.shape[2:], act.dtype)

        @pl.when(col == 0)
        def _():
            act[buf, pl.ds(0, rows + 2), 0] = jnp.zeros((rows + 2,) + act.shape[3:], act.dtype)

        @pl.when(col == col_devs - 1)
        def _():
            act[buf, pl.ds(0, rows + 2), cols + 1] = jnp.zeros((rows + 2,) + act.shape[3:], act.dtype)
        return carry

    lax.fori_loop(0, layers * GROUPS, zero_borders, 0)

    block = imgs * imgs
    out_row = lax.broadcasted_iota(jnp.int32, (block, block), 0)
    in_row = lax.broadcasted_iota(jnp.int32, (block, block), 1)
    swapped = (out_row % imgs) * imgs + out_row // imgs
    perm[...] = jnp.where(in_row == swapped, 1.0, 0.0).astype(jnp.bfloat16)

    pl.semaphore_wait(barrier, len(NBRS))

    def put(buf, r, first, count, y):
        for hf in range(halves):
            act[buf, r + 1, pl.ds(first + 1, count), hf] = y[:, hf * LANES:(hf + 1) * LANES].reshape(count, imgs, LANES)

    order = (0, rows - 1) + tuple(range(1, rows - 1))
    for g in range(GROUPS):
        for hf in range(halves):
            x_copies[g * halves + hf].wait()
        for i, r in enumerate(order):
            for first in range(0, cols, imgs):
                tile = jnp.concatenate([x_vm[g, hf, :, r, pl.ds(first, imgs)].reshape(block, LANES) for hf in range(halves)], axis=1)
                y = jnp.dot(perm[...], tile, preferred_element_type=jnp.float32)
                put(g, r, first, imgs, y.astype(jnp.bfloat16))
            if i == 1:
                send(g, ROW_SENDS)
        send(g, COL_SENDS)
    for c in w_copies + [b_copy]:
        c.wait()

    def conv(taps, layer):
        lhs = jnp.concatenate([tap[..., hf, :, :].reshape(-1, LANES) for tap in taps for hf in range(halves)], axis=1)
        wt = jnp.concatenate([w_vm[layer, hf] for hf in range(halves)], axis=1)
        y = jnp.dot(lhs, wt, preferred_element_type=jnp.float32)
        return jnp.maximum(y + b_ref[pl.ds(layer, 1), :], 0.0)

    def conv_row(p, layer, r, first, count):
        return conv([act[p, r + t // 3, pl.ds(first + t % 3, count)] for t in range(TAPS)], layer)

    def first_layer(g, carry):
        for r in range(1, rows - 1):
            y = conv_row(g, 0, r, 1, cols - 2)
            put(g + GROUPS, r, 1, cols - 2, y.astype(jnp.bfloat16))
        receive(g)
        edge = cols * imgs
        for r, c in ((0, 0), (rows - 1, cols - 1)):
            taps = []
            for t in range(TAPS):
                line = act[g, r + t // 3, pl.ds(t % 3, cols)]
                side = act[g, pl.ds(1 + t // 3, rows - 2), c + t % 3]
                taps.append(jnp.concatenate([line, side], axis=0))
            y = conv(taps, 0).astype(jnp.bfloat16)
            put(g + GROUPS, r, 0, cols, y[:edge])
            for hf in range(halves):
                act[g + GROUPS, pl.ds(2, rows - 2), c + 1, hf] = y[edge:, hf * LANES:(hf + 1) * LANES].reshape(rows - 2, imgs, LANES)
        send(g + GROUPS, ROW_SENDS + COL_SENDS)
        return carry

    lax.fori_loop(0, GROUPS, first_layer, 0)

    def middle_layer(p, carry):
        receive(p)
        for i, r in enumerate(order):
            y = conv_row(p, p // GROUPS, r, 0, cols)
            put(p + GROUPS, r, 0, cols, y.astype(jnp.bfloat16))
            if i == 1:
                send(p + GROUPS, ROW_SENDS)
        send(p + GROUPS, COL_SENDS)
        return carry

    lax.fori_loop(GROUPS, (layers - 1) * GROUPS, middle_layer, 0)

    def last_layer(g, carry):
        p = (layers - 1) * GROUPS + g
        receive(p)
        for r in range(rows):
            y = conv_row(p, layers - 1, r, 0, cols)
            for c in range(cols):
                for hf in range(halves):
                    turn[r % 2, hf, pl.ds(c, imgs, stride=pitch), :] = y[c * imgs:(c + 1) * imgs, hf * LANES:(hf + 1) * LANES]
            for i in range(imgs):
                for hf in range(halves):
                    line = turn[r % 2, hf, pl.ds(i * pitch, cols), :].astype(jnp.bfloat16)
                    o_ref[g * imgs + i, r, :, pl.ds(hf * LANES, LANES)] = line
        return carry

    lax.fori_loop(0, GROUPS, last_layer, 0)

    def finish(buf, carry):
        for n in range(len(NBRS)):
            edge_copy(buf, n).wait_send()
        return carry

    lax.fori_loop(0, layers * GROUPS, finish, 0)


def solution(mesh):
    row_devs = mesh.shape["row"]
    col_devs = mesh.shape["col"]
    act_spec = P("ens", "row", "col", None)

    def local_stack(x_tile, weights, biases):
        batch, rows, cols, ch = x_tile.shape
        layers = weights.shape[0]
        imgs = batch // GROUPS
        halves = ch // LANES
        dims = (layers, imgs, rows, cols, ch, row_devs, col_devs)
        hbm = pl.BlockSpec(memory_space=pltpu.HBM)
        return pl.pallas_call(
            functools.partial(kernel, dims),
            out_shape=pltpu.VMEM((batch, rows, cols, ch), jnp.bfloat16),
            in_specs=[hbm, hbm, hbm],
            out_specs=pl.BlockSpec(memory_space=pltpu.VMEM),
            scratch_shapes=[
                pltpu.VMEM((layers * GROUPS, rows + 3, cols + 3, halves, imgs, LANES), jnp.bfloat16),
                pltpu.VMEM((layers, halves, TAPS * ch, LANES), jnp.bfloat16),
                pltpu.VMEM((layers, ch), jnp.float32),
                pltpu.VMEM((GROUPS, halves, imgs, rows, cols, LANES), jnp.bfloat16),
                pltpu.VMEM((imgs * imgs, imgs * imgs), jnp.bfloat16),
                pltpu.VMEM((2, halves, imgs * (cols + 8), LANES), jnp.float32),
                pltpu.SemaphoreType.DMA(((GROUPS + layers) * halves + 1,)),
                pltpu.SemaphoreType.DMA((layers * GROUPS, len(NBRS))),
                pltpu.SemaphoreType.DMA((layers * GROUPS, len(NBRS))),
            ],
            compiler_params=pltpu.CompilerParams(collective_id=0, has_side_effects=True, vmem_limit_bytes=56 * 1024 * 1024),
            name="conv_stack",
        )(x_tile, weights.reshape(layers, TAPS * ch, ch), biases)

    return jax.shard_map(local_stack, mesh=mesh, in_specs=(act_spec, P(), P()), out_specs=act_spec, check_vma=False)
```

```python
import functools

import jax
import jax.numpy as jnp
from jax import lax
from jax.experimental import pallas as pl
from jax.experimental.pallas import tpu as pltpu
from jax.sharding import PartitionSpec as P

MESH = pl.DeviceIdType.MESH
LANES = 128
GROUPS = 2
TAPS = 9
NBRS = ((-1, 0), (1, 0), (0, -1), (0, 1), (-1, -1), (-1, 1), (1, -1), (1, 1))
ROW_SENDS = (0, 1, 4, 5, 6, 7)
COL_SENDS = (2, 3)


def kernel(dims, x_hbm, w_hbm, b_hbm, o_ref, act, w_vm, b_ref, x_vm, perm, turn, in_sem, send_sem, recv_sem):
    layers, imgs, rows, cols, ch, row_devs, col_devs = dims
    halves = ch // LANES
    pitch = cols + 8
    row, col = lax.axis_index("row"), lax.axis_index("col")

    has = {(-1, 0): row > 0, (1, 0): row < row_devs - 1, (0, -1): col > 0, (0, 1): col < col_devs - 1}

    def exists(dr, dc):
        if dr and dc:
            return jnp.logical_and(has[(dr, 0)], has[(0, dc)])
        return has[(dr, dc)]

    def span(step, size):
        if step < 0:
            return pl.ds(1, 1), pl.ds(size + 1, 1)
        if step > 0:
            return pl.ds(size, 1), pl.ds(0, 1)
        return pl.ds(1, size), pl.ds(1, size)

    def neighbour(n):
        return {"row": row + NBRS[n][0], "col": col + NBRS[n][1]}

    def edge_copy(buf, n):
        src_r, dst_r = span(NBRS[n][0], rows)
        src_c, dst_c = span(NBRS[n][1], cols)
        return pltpu.make_async_remote_copy(
            src_ref=act.at[buf, src_r, src_c],
            dst_ref=act.at[buf, dst_r, dst_c],
            send_sem=send_sem.at[buf, n],
            recv_sem=recv_sem.at[buf, n],
            device_id=neighbour(n),
            device_id_type=MESH,
        )

    def send(buf, which):
        for n in which:
            @pl.when(exists(*NBRS[n]))
            def _(n=n):
                edge_copy(buf, n).start()

    def receive(buf):
        for n, (dr, dc) in enumerate(NBRS):
            @pl.when(exists(-dr, -dc))
            def _(n=n):
                edge_copy(buf, n).wait_recv()

    x_copies, w_copies = [], []
    for g in range(GROUPS):
        for hf in range(halves):
            x_copies.append(pltpu.make_async_copy(
                x_hbm.at[pl.ds(g * imgs, imgs), :, :, pl.ds(hf * LANES, LANES)], x_vm.at[g, hf], in_sem.at[g * halves + hf]))
    for l in range(layers):
        for hf in range(halves):
            w_copies.append(pltpu.make_async_copy(
                w_hbm.at[l, :, pl.ds(hf * LANES, LANES)], w_vm.at[l, hf], in_sem.at[(GROUPS + l) * halves + hf]))
    b_copy = pltpu.make_async_copy(b_hbm, b_ref, in_sem.at[(GROUPS + layers) * halves])
    for c in x_copies[:halves]:
        c.start()

    barrier = pltpu.get_barrier_semaphore()
    for n in range(len(NBRS)):
        @pl.when(exists(*NBRS[n]))
        def _(n=n):
            pl.semaphore_signal(barrier, inc=1, device_id=neighbour(n), device_id_type=MESH)

    def zero_borders(buf, carry):
        @pl.when(row == 0)
        def _():
            act[buf, 0] = jnp.zeros(act.shape[2:], act.dtype)

        @pl.when(row == row_devs - 1)
        def _():
            act[buf, rows + 1] = jnp.zeros(act.shape[2:], act.dtype)

        @pl.when(col == 0)
        def _():
            act[buf, pl.ds(0, rows + 2), 0] = jnp.zeros((rows + 2,) + act.shape[3:], act.dtype)

        @pl.when(col == col_devs - 1)
        def _():
            act[buf, pl.ds(0, rows + 2), cols + 1] = jnp.zeros((rows + 2,) + act.shape[3:], act.dtype)
        return carry

    lax.fori_loop(0, layers * GROUPS, zero_borders, 0)

    block = imgs * imgs
    out_row = lax.broadcasted_iota(jnp.int32, (block, block), 0)
    in_row = lax.broadcasted_iota(jnp.int32, (block, block), 1)
    swapped = (out_row % imgs) * imgs + out_row // imgs
    perm[...] = jnp.where(in_row == swapped, 1.0, 0.0).astype(jnp.bfloat16)

    n_row = 1 + sum(has[(d, 0)].astype(jnp.int32) for d in (-1, 1))
    n_col = 1 + sum(has[(0, d)].astype(jnp.int32) for d in (-1, 1))
    pl.semaphore_wait(barrier, n_row * n_col - 1)

    def put(buf, r, first, count, y):
        for hf in range(halves):
            act[buf, r + 1, pl.ds(first + 1, count), hf] = y[:, hf * LANES:(hf + 1) * LANES].reshape(count, imgs, LANES)

    order = (0, rows - 1) + tuple(range(1, rows - 1))
    for g in range(GROUPS):
        for hf in range(halves):
            x_copies[g * halves + hf].wait()
        if g == 0:
            for c in x_copies[halves:] + w_copies + [b_copy]:
                c.start()
        for i, r in enumerate(order):
            for first in range(0, cols, imgs):
                tile = jnp.concatenate([x_vm[g, hf, :, r, pl.ds(first, imgs)].reshape(block, LANES) for hf in range(halves)], axis=1)
                y = jnp.dot(perm[...], tile, preferred_element_type=jnp.float32)
                put(g, r, first, imgs, y.astype(jnp.bfloat16))
            if i == 1:
                send(g, ROW_SENDS)
        send(g, COL_SENDS)
    for c in w_copies + [b_copy]:
        c.wait()

    def conv(taps, layer):
        lhs = jnp.concatenate([tap[..., hf, :, :].reshape(-1, LANES) for tap in taps for hf in range(halves)], axis=1)
        wt = jnp.concatenate([w_vm[layer, hf] for hf in range(halves)], axis=1)
        y = jnp.dot(lhs, wt, preferred_element_type=jnp.float32)
        return jnp.maximum(y + b_ref[pl.ds(layer, 1), :], 0.0)

    def conv_row(p, layer, r, first, count):
        return conv([act[p, r + t // 3, pl.ds(first + t % 3, count)] for t in range(TAPS)], layer)

    def first_layer(g, carry):
        for r in range(1, rows - 1):
            y = conv_row(g, 0, r, 1, cols - 2)
            put(g + GROUPS, r, 1, cols - 2, y.astype(jnp.bfloat16))
        receive(g)
        edge = cols * imgs
        for r, c in ((0, 0), (rows - 1, cols - 1)):
            taps = []
            for t in range(TAPS):
                line = act[g, r + t // 3, pl.ds(t % 3, cols)]
                side = act[g, pl.ds(1 + t // 3, rows - 2), c + t % 3]
                taps.append(jnp.concatenate([line, side], axis=0))
            y = conv(taps, 0).astype(jnp.bfloat16)
            put(g + GROUPS, r, 0, cols, y[:edge])
            for hf in range(halves):
                act[g + GROUPS, pl.ds(2, rows - 2), c + 1, hf] = y[edge:, hf * LANES:(hf + 1) * LANES].reshape(rows - 2, imgs, LANES)
        send(g + GROUPS, ROW_SENDS + COL_SENDS)
        return carry

    lax.fori_loop(0, GROUPS, first_layer, 0)

    def middle_layer(p, carry):
        receive(p)
        for i, r in enumerate(order):
            y = conv_row(p, p // GROUPS, r, 0, cols)
            put(p + GROUPS, r, 0, cols, y.astype(jnp.bfloat16))
            if i == 1:
                send(p + GROUPS, ROW_SENDS)
        send(p + GROUPS, COL_SENDS)
        return carry

    lax.fori_loop(GROUPS, (layers - 1) * GROUPS, middle_layer, 0)

    def last_layer(g, carry):
        p = (layers - 1) * GROUPS + g
        receive(p)
        for r in range(rows):
            y = conv_row(p, layers - 1, r, 0, cols)
            for c in range(cols):
                for hf in range(halves):
                    turn[r % 2, hf, pl.ds(c, imgs, stride=pitch), :] = y[c * imgs:(c + 1) * imgs, hf * LANES:(hf + 1) * LANES]
            for i in range(imgs):
                for hf in range(halves):
                    line = turn[r % 2, hf, pl.ds(i * pitch, cols), :].astype(jnp.bfloat16)
                    o_ref[g * imgs + i, r, :, pl.ds(hf * LANES, LANES)] = line
        return carry

    lax.fori_loop(0, GROUPS, last_layer, 0)

    def finish(buf, carry):
        for n in range(len(NBRS)):
            @pl.when(exists(*NBRS[n]))
            def _(n=n):
                edge_copy(buf, n).wait_send()
        return carry

    lax.fori_loop(0, layers * GROUPS, finish, 0)


def solution(mesh):
    row_devs = mesh.shape["row"]
    col_devs = mesh.shape["col"]
    act_spec = P("ens", "row", "col", None)

    def local_stack(x_tile, weights, biases):
        batch, rows, cols, ch = x_tile.shape
        layers = weights.shape[0]
        imgs = batch // GROUPS
        halves = ch // LANES
        dims = (layers, imgs, rows, cols, ch, row_devs, col_devs)
        hbm = pl.BlockSpec(memory_space=pltpu.HBM)
        return pl.pallas_call(
            functools.partial(kernel, dims),
            out_shape=pltpu.VMEM((batch, rows, cols, ch), jnp.bfloat16),
            in_specs=[hbm, hbm, hbm],
            out_specs=pl.BlockSpec(memory_space=pltpu.VMEM),
            scratch_shapes=[
                pltpu.VMEM((layers * GROUPS, rows + 2, cols + 2, halves, imgs, LANES), jnp.bfloat16),
                pltpu.VMEM((layers, halves, TAPS * ch, LANES), jnp.bfloat16),
                pltpu.VMEM((layers, ch), jnp.float32),
                pltpu.VMEM((GROUPS, halves, imgs, rows, cols, LANES), jnp.bfloat16),
                pltpu.VMEM((imgs * imgs, imgs * imgs), jnp.bfloat16),
                pltpu.VMEM((2, halves, imgs * (cols + 8), LANES), jnp.float32),
                pltpu.SemaphoreType.DMA(((GROUPS + layers) * halves + 1,)),
                pltpu.SemaphoreType.DMA((layers * GROUPS, len(NBRS))),
                pltpu.SemaphoreType.DMA((layers * GROUPS, len(NBRS))),
            ],
            compiler_params=pltpu.CompilerParams(collective_id=0, has_side_effects=True, vmem_limit_bytes=56 * 1024 * 1024),
            name="conv_stack",
        )(x_tile, weights.reshape(layers, TAPS * ch, ch), biases)

    return jax.shard_map(local_stack, mesh=mesh, in_specs=(act_spec, P(), P()), out_specs=act_spec, check_vma=False)
```

```python
import functools

import jax
import jax.numpy as jnp
from jax import lax
from jax.experimental import pallas as pl
from jax.experimental.pallas import tpu as pltpu
from jax.sharding import PartitionSpec as P

MESH = pl.DeviceIdType.MESH
LANES = 128
GROUPS = 2
TAPS = 9
NBRS = ((-1, 0), (1, 0), (0, -1), (0, 1), (-1, -1), (-1, 1), (1, -1), (1, 1))
SEND_ORDER = (4, 5, 6, 7, 2, 3, 0, 1)
EARLY_ROWS = 2


def kernel(dims, x_hbm, w_hbm, b_hbm, o_ref, act, w_vm, b_ref, x_vm, perm, turn, in_sem, send_sem, recv_sem):
    layers, imgs, rows, cols, ch, row_devs, col_devs = dims
    halves = ch // LANES
    pitch = cols + 8
    row, col = lax.axis_index("row"), lax.axis_index("col")

    has = {(-1, 0): row > 0, (1, 0): row < row_devs - 1, (0, -1): col > 0, (0, 1): col < col_devs - 1}

    def exists(dr, dc):
        if dr and dc:
            return jnp.logical_and(has[(dr, 0)], has[(0, dc)])
        return has[(dr, dc)]

    def span(step, size):
        if step < 0:
            return pl.ds(1, 1), pl.ds(size + 1, 1)
        if step > 0:
            return pl.ds(size, 1), pl.ds(0, 1)
        return pl.ds(1, size), pl.ds(1, size)

    def neighbour(n):
        return {"row": row + NBRS[n][0], "col": col + NBRS[n][1]}

    def edge_copy(buf, n):
        src_r, dst_r = span(NBRS[n][0], rows)
        src_c, dst_c = span(NBRS[n][1], cols)
        return pltpu.make_async_remote_copy(
            src_ref=act.at[buf, src_r, src_c],
            dst_ref=act.at[buf, dst_r, dst_c],
            send_sem=send_sem.at[buf, n],
            recv_sem=recv_sem.at[buf, n],
            device_id=neighbour(n),
            device_id_type=MESH,
        )

    def send(buf):
        for n in SEND_ORDER:
            @pl.when(exists(*NBRS[n]))
            def _(n=n):
                edge_copy(buf, n).start()

    def receive(buf):
        for n, (dr, dc) in enumerate(NBRS):
            @pl.when(exists(-dr, -dc))
            def _(n=n):
                edge_copy(buf, n).wait_recv()

    x_copies, w_copies = [], []
    for g in range(GROUPS):
        for hf in range(halves):
            x_copies.append(pltpu.make_async_copy(
                x_hbm.at[pl.ds(g * imgs, imgs), :, :, pl.ds(hf * LANES, LANES)], x_vm.at[g, hf], in_sem.at[g * halves + hf]))
    for l in range(layers):
        for hf in range(halves):
            w_copies.append(pltpu.make_async_copy(
                w_hbm.at[l, :, pl.ds(hf * LANES, LANES)], w_vm.at[l, hf], in_sem.at[(GROUPS + l) * halves + hf]))
    b_copy = pltpu.make_async_copy(b_hbm, b_ref, in_sem.at[(GROUPS + layers) * halves])
    for c in x_copies[:halves] + w_copies[:halves] + [b_copy]:
        c.start()

    barrier = pltpu.get_barrier_semaphore()
    for n in range(len(NBRS)):
        @pl.when(exists(*NBRS[n]))
        def _(n=n):
            pl.semaphore_signal(barrier, inc=1, device_id=neighbour(n), device_id_type=MESH)

    def zero_borders(buf, carry):
        @pl.when(row == 0)
        def _():
            act[buf, 0] = jnp.zeros(act.shape[2:], act.dtype)

        @pl.when(row == row_devs - 1)
        def _():
            act[buf, rows + 1] = jnp.zeros(act.shape[2:], act.dtype)

        @pl.when(col == 0)
        def _():
            act[buf, pl.ds(0, rows + 2), 0] = jnp.zeros((rows + 2,) + act.shape[3:], act.dtype)

        @pl.when(col == col_devs - 1)
        def _():
            act[buf, pl.ds(0, rows + 2), cols + 1] = jnp.zeros((rows + 2,) + act.shape[3:], act.dtype)
        return carry

    lax.fori_loop(0, layers * GROUPS, zero_borders, 0)

    block = imgs * imgs
    out_row = lax.broadcasted_iota(jnp.int32, (block, block), 0)
    in_row = lax.broadcasted_iota(jnp.int32, (block, block), 1)
    swapped = (out_row % imgs) * imgs + out_row // imgs
    perm[...] = jnp.where(in_row == swapped, 1.0, 0.0).astype(jnp.bfloat16)

    for c in x_copies[halves:]:
        c.start()

    def put(buf, r, first, count, y):
        for hf in range(halves):
            act[buf, r + 1, pl.ds(first + 1, count), hf] = y[:, hf * LANES:(hf + 1) * LANES].reshape(count, imgs, LANES)

    order = (0, rows - 1) + tuple(range(1, rows - 1))

    def turn_input(g):
        for hf in range(halves):
            x_copies[g * halves + hf].wait()
        for r in order:
            for first in range(0, cols, imgs):
                tile = jnp.concatenate([x_vm[g, hf, :, r, pl.ds(first, imgs)].reshape(block, LANES) for hf in range(halves)], axis=1)
                y = jnp.dot(perm[...], tile, preferred_element_type=jnp.float32)
                put(g, r, first, imgs, y.astype(jnp.bfloat16))

    def conv(taps, layer):
        lhs = jnp.concatenate([tap[..., hf, :, :].reshape(-1, LANES) for tap in taps for hf in range(halves)], axis=1)
        wt = jnp.concatenate([w_vm[layer, hf] for hf in range(halves)], axis=1)
        y = jnp.dot(lhs, wt, preferred_element_type=jnp.float32)
        return jnp.maximum(y + b_ref[pl.ds(layer, 1), :], 0.0)

    def conv_row(p, layer, r, first, count):
        return conv([act[p, r + t // 3, pl.ds(first + t % 3, count)] for t in range(TAPS)], layer)

    def keep(buf, r, first, count, y):
        put(buf, r, first, count, y.astype(jnp.bfloat16))

    def keep_last(buf, r, first, count, y):
        for i in range(count):
            for hf in range(halves):
                turn[buf - layers * GROUPS, r, hf, pl.ds(first + i, imgs, stride=pitch), :] = y[i * imgs:(i + 1) * imgs, hf * LANES:(hf + 1) * LANES]

    def write_row(g, r):
        for i in range(imgs):
            for hf in range(halves):
                line = turn[g, r, hf, pl.ds(i * pitch, cols), :].astype(jnp.bfloat16)
                o_ref[g * imgs + i, r, :, pl.ds(hf * LANES, LANES)] = line

    def interior(p, which, store):
        for r in which:
            store(p + GROUPS, r, 1, cols - 2, conv_row(p, p // GROUPS, r, 1, cols - 2))

    def side_taps(p, c):
        return [act[p, pl.ds(1 + t // 3, rows - 2), c + t % 3] for t in range(TAPS)]

    inner = range(1, rows - 1)
    corners = ((0, 0), (rows - 1, cols - 1))

    def edges(p):
        edge = cols * imgs
        for r, c in corners:
            side = side_taps(p, c)
            taps = [jnp.concatenate([act[p, r + t // 3, pl.ds(t % 3, cols)], side[t]], axis=0) for t in range(TAPS)]
            y = conv(taps, p // GROUPS).astype(jnp.bfloat16)
            put(p + GROUPS, r, 0, cols, y[:edge])
            for hf in range(halves):
                act[p + GROUPS, pl.ds(2, rows - 2), c + 1, hf] = y[edge:, hf * LANES:(hf + 1) * LANES].reshape(rows - 2, imgs, LANES)

    turn_input(0)
    turn_input(1)
    for c in w_copies[:halves] + [b_copy]:
        c.wait()
    interior(0, inner[:EARLY_ROWS], keep)
    n_row = 1 + sum(has[(d, 0)].astype(jnp.int32) for d in (-1, 1))
    n_col = 1 + sum(has[(0, d)].astype(jnp.int32) for d in (-1, 1))
    pl.semaphore_wait(barrier, n_row * n_col - 1)
    for g in range(GROUPS):
        send(g)
    for c in w_copies[halves:]:
        c.start()
    interior(0, inner[EARLY_ROWS:], keep)
    interior(1, inner, keep)
    for c in w_copies[halves:]:
        c.wait()

    def middle(p, carry):
        receive(p)
        edges(p)
        send(p + GROUPS)
        interior(p + GROUPS, inner, keep)
        return carry

    lax.fori_loop(0, (layers - 2) * GROUPS, middle, 0)

    def next_to_last(p, carry):
        receive(p)
        edges(p)
        send(p + GROUPS)
        interior(p + GROUPS, inner, keep_last)
        return carry

    lax.fori_loop((layers - 2) * GROUPS, (layers - 1) * GROUPS, next_to_last, 0)

    def last(g, carry):
        p = (layers - 1) * GROUPS + g
        receive(p)
        for _, c in corners:
            y = conv(side_taps(p, c), layers - 1)
            for i in range(rows - 2):
                keep_last(p + GROUPS, i + 1, c, 1, y[i * imgs:(i + 1) * imgs])
        for r, _ in corners:
            keep_last(p + GROUPS, r, 0, cols, conv_row(p, layers - 1, r, 0, cols))
            if r == 0:
                for i in inner:
                    write_row(g, i)
        for r, _ in corners:
            write_row(g, r)
        return carry

    lax.fori_loop(0, GROUPS, last, 0)

    def finish(buf, carry):
        for n in range(len(NBRS)):
            @pl.when(exists(*NBRS[n]))
            def _(n=n):
                edge_copy(buf, n).wait_send()
        return carry

    lax.fori_loop(0, layers * GROUPS, finish, 0)


def solution(mesh):
    row_devs = mesh.shape["row"]
    col_devs = mesh.shape["col"]
    act_spec = P("ens", "row", "col", None)

    def local_stack(x_tile, weights, biases):
        batch, rows, cols, ch = x_tile.shape
        layers = weights.shape[0]
        imgs = batch // GROUPS
        halves = ch // LANES
        dims = (layers, imgs, rows, cols, ch, row_devs, col_devs)
        hbm = pl.BlockSpec(memory_space=pltpu.HBM)
        return pl.pallas_call(
            functools.partial(kernel, dims),
            out_shape=pltpu.VMEM((batch, rows, cols, ch), jnp.bfloat16),
            in_specs=[hbm, hbm, hbm],
            out_specs=pl.BlockSpec(memory_space=pltpu.VMEM),
            scratch_shapes=[
                pltpu.VMEM((layers * GROUPS, rows + 2, cols + 2, halves, imgs, LANES), jnp.bfloat16),
                pltpu.VMEM((layers, halves, TAPS * ch, LANES), jnp.bfloat16),
                pltpu.VMEM((layers, ch), jnp.float32),
                pltpu.VMEM((GROUPS, halves, imgs, rows, cols, LANES), jnp.bfloat16),
                pltpu.VMEM((imgs * imgs, imgs * imgs), jnp.bfloat16),
                pltpu.VMEM((GROUPS, rows, halves, imgs * (cols + 8), LANES), jnp.float32),
                pltpu.SemaphoreType.DMA(((GROUPS + layers) * halves + 1,)),
                pltpu.SemaphoreType.DMA((layers * GROUPS, len(NBRS))),
                pltpu.SemaphoreType.DMA((layers * GROUPS, len(NBRS))),
            ],
            compiler_params=pltpu.CompilerParams(collective_id=0, has_side_effects=True, vmem_limit_bytes=56 * 1024 * 1024),
            name="conv_stack",
        )(x_tile, weights.reshape(layers, TAPS * ch, ch), biases)

    return jax.shard_map(local_stack, mesh=mesh, in_specs=(act_spec, P(), P()), out_specs=act_spec, check_vma=False)
```

```python
import functools

import jax
import jax.numpy as jnp
from jax import lax
from jax.experimental import pallas as pl
from jax.experimental.pallas import tpu as pltpu
from jax.sharding import PartitionSpec as P

MESH = pl.DeviceIdType.MESH
LANES = 128
GROUPS = 2
TAPS = 9
NBRS = ((-1, 0), (1, 0), (0, -1), (0, 1), (-1, -1), (-1, 1), (1, -1), (1, 1))
SEND_ORDER = (4, 5, 6, 7, 2, 3, 0, 1)
EARLY_ROWS = 2


def kernel(dims, x_hbm, w_hbm, b_hbm, o_ref, act, w_vm, b_ref, x_vm, perm, turn, in_sem, send_sem, recv_sem):
    layers, imgs, rows, cols, ch, row_devs, col_devs = dims
    halves = ch // LANES
    pitch = cols + 1
    row, col = lax.axis_index("row"), lax.axis_index("col")

    has = {(-1, 0): row > 0, (1, 0): row < row_devs - 1, (0, -1): col > 0, (0, 1): col < col_devs - 1}

    def exists(dr, dc):
        if dr and dc:
            return jnp.logical_and(has[(dr, 0)], has[(0, dc)])
        return has[(dr, dc)]

    def span(step, size):
        if step < 0:
            return pl.ds(1, 1), pl.ds(size + 1, 1)
        if step > 0:
            return pl.ds(size, 1), pl.ds(0, 1)
        return pl.ds(1, size), pl.ds(1, size)

    def neighbour(n):
        return {"row": row + NBRS[n][0], "col": col + NBRS[n][1]}

    def edge_copy(buf, n):
        src_r, dst_r = span(NBRS[n][0], rows)
        src_c, dst_c = span(NBRS[n][1], cols)
        return pltpu.make_async_remote_copy(
            src_ref=act.at[buf, src_r, src_c],
            dst_ref=act.at[buf, dst_r, dst_c],
            send_sem=send_sem.at[buf, n],
            recv_sem=recv_sem.at[buf, n],
            device_id=neighbour(n),
            device_id_type=MESH,
        )

    def send(buf):
        for n in SEND_ORDER:
            @pl.when(exists(*NBRS[n]))
            def _(n=n):
                edge_copy(buf, n).start()

    def receive(buf):
        for n, (dr, dc) in enumerate(NBRS):
            @pl.when(exists(-dr, -dc))
            def _(n=n):
                edge_copy(buf, n).wait_recv()

    x_copies, w_copies = [], []
    for g in range(GROUPS):
        for hf in range(halves):
            x_copies.append(pltpu.make_async_copy(
                x_hbm.at[pl.ds(g * imgs, imgs), :, :, pl.ds(hf * LANES, LANES)], x_vm.at[g, hf], in_sem.at[g * halves + hf]))
    for l in range(layers):
        for hf in range(halves):
            w_copies.append(pltpu.make_async_copy(
                w_hbm.at[l, :, pl.ds(hf * LANES, LANES)], w_vm.at[l, hf], in_sem.at[(GROUPS + l) * halves + hf]))
    b_copy = pltpu.make_async_copy(b_hbm, b_ref, in_sem.at[(GROUPS + layers) * halves])
    for c in x_copies[:halves] + w_copies[:halves] + [b_copy]:
        c.start()

    barrier = pltpu.get_barrier_semaphore()
    for n in range(len(NBRS)):
        @pl.when(exists(*NBRS[n]))
        def _(n=n):
            pl.semaphore_signal(barrier, inc=1, device_id=neighbour(n), device_id_type=MESH)

    def zero_borders(buf, carry):
        @pl.when(row == 0)
        def _():
            act[buf, 0] = jnp.zeros(act.shape[2:], act.dtype)

        @pl.when(row == row_devs - 1)
        def _():
            act[buf, rows + 1] = jnp.zeros(act.shape[2:], act.dtype)

        @pl.when(col == 0)
        def _():
            act[buf, pl.ds(0, rows + 2), 0] = jnp.zeros((rows + 2,) + act.shape[3:], act.dtype)

        @pl.when(col == col_devs - 1)
        def _():
            act[buf, pl.ds(0, rows + 2), cols + 1] = jnp.zeros((rows + 2,) + act.shape[3:], act.dtype)
        return carry

    lax.fori_loop(0, layers * GROUPS, zero_borders, 0)

    block = imgs * imgs
    out_row = lax.broadcasted_iota(jnp.int32, (block, block), 0)
    in_row = lax.broadcasted_iota(jnp.int32, (block, block), 1)
    swapped = (out_row % imgs) * imgs + out_row // imgs
    perm[...] = jnp.where(in_row == swapped, 1.0, 0.0).astype(jnp.bfloat16)

    for c in x_copies[halves:]:
        c.start()

    def put(buf, r, first, count, y):
        for hf in range(halves):
            act[buf, r + 1, pl.ds(first + 1, count), hf] = y[:, hf * LANES:(hf + 1) * LANES].reshape(count, imgs, LANES)

    order = (0, rows - 1) + tuple(range(1, rows - 1))

    def turn_input(g):
        for hf in range(halves):
            x_copies[g * halves + hf].wait()
        for r in order:
            for first in range(0, cols, imgs):
                tile = jnp.concatenate([x_vm[g, hf, :, r, pl.ds(first, imgs)].reshape(block, LANES) for hf in range(halves)], axis=1)
                y = jnp.dot(perm[...], tile, preferred_element_type=jnp.float32)
                put(g, r, first, imgs, y.astype(jnp.bfloat16))

    def conv(taps, layer):
        lhs = jnp.concatenate([tap[..., hf, :, :].reshape(-1, LANES) for tap in taps for hf in range(halves)], axis=1)
        wt = jnp.concatenate([w_vm[layer, hf] for hf in range(halves)], axis=1)
        y = jnp.dot(lhs, wt, preferred_element_type=jnp.float32)
        return jnp.maximum(y + b_ref[pl.ds(layer, 1), :], 0.0)

    def conv_row(p, layer, r, first, count):
        return conv([act[p, r + t // 3, pl.ds(first + t % 3, count)] for t in range(TAPS)], layer)

    def keep(buf, r, first, count, y):
        put(buf, r, first, count, y.astype(jnp.bfloat16))

    def keep_last(buf, r, first, count, y):
        for i in range(count):
            for hf in range(halves):
                turn[buf - layers * GROUPS, r, hf, pl.ds(first + i, imgs, stride=pitch), :] = y[i * imgs:(i + 1) * imgs, hf * LANES:(hf + 1) * LANES]

    def write_row(g, r):
        for i in range(imgs):
            for hf in range(halves):
                line = turn[g, r, hf, pl.ds(i * pitch, cols), :].astype(jnp.bfloat16)
                o_ref[g * imgs + i, r, :, pl.ds(hf * LANES, LANES)] = line

    def interior(p, which, store):
        for r in which:
            store(p + GROUPS, r, 1, cols - 2, conv_row(p, p // GROUPS, r, 1, cols - 2))

    def side_taps(p, c):
        return [act[p, pl.ds(1 + t // 3, rows - 2), c + t % 3] for t in range(TAPS)]

    inner = range(1, rows - 1)
    corners = ((0, 0), (rows - 1, cols - 1))

    def edges(p):
        edge = cols * imgs
        for r, c in corners:
            side = side_taps(p, c)
            taps = [jnp.concatenate([act[p, r + t // 3, pl.ds(t % 3, cols)], side[t]], axis=0) for t in range(TAPS)]
            y = conv(taps, p // GROUPS).astype(jnp.bfloat16)
            put(p + GROUPS, r, 0, cols, y[:edge])
            for hf in range(halves):
                act[p + GROUPS, pl.ds(2, rows - 2), c + 1, hf] = y[edge:, hf * LANES:(hf + 1) * LANES].reshape(rows - 2, imgs, LANES)

    turn_input(0)
    turn_input(1)
    for c in w_copies[:halves] + [b_copy]:
        c.wait()
    interior(0, inner[:EARLY_ROWS], keep)
    n_row = 1 + sum(has[(d, 0)].astype(jnp.int32) for d in (-1, 1))
    n_col = 1 + sum(has[(0, d)].astype(jnp.int32) for d in (-1, 1))
    pl.semaphore_wait(barrier, n_row * n_col - 1)
    for g in range(GROUPS):
        send(g)
    for c in w_copies[halves:]:
        c.start()
    interior(0, inner[EARLY_ROWS:], keep)
    interior(1, inner, keep)
    for c in w_copies[halves:]:
        c.wait()

    def middle(p, carry):
        receive(p)
        edges(p)
        send(p + GROUPS)
        interior(p + GROUPS, inner, keep)
        return carry

    lax.fori_loop(0, (layers - 2) * GROUPS, middle, 0)

    def next_to_last(p, carry):
        receive(p)
        edges(p)
        send(p + GROUPS)
        interior(p + GROUPS, inner, keep_last)
        return carry

    lax.fori_loop((layers - 2) * GROUPS, (layers - 1) * GROUPS, next_to_last, 0)

    def last(g, carry):
        p = (layers - 1) * GROUPS + g
        receive(p)
        for _, c in corners:
            y = conv(side_taps(p, c), layers - 1)
            for i in range(rows - 2):
                keep_last(p + GROUPS, i + 1, c, 1, y[i * imgs:(i + 1) * imgs])
        for r, _ in corners:
            keep_last(p + GROUPS, r, 0, cols, conv_row(p, layers - 1, r, 0, cols))
            if r == 0:
                for i in inner:
                    write_row(g, i)
        for r, _ in corners:
            write_row(g, r)
        return carry

    lax.fori_loop(0, GROUPS, last, 0)

    def finish(buf, carry):
        for n in range(len(NBRS)):
            @pl.when(exists(*NBRS[n]))
            def _(n=n):
                edge_copy(buf, n).wait_send()
        return carry

    lax.fori_loop(0, layers * GROUPS, finish, 0)


def solution(mesh):
    row_devs = mesh.shape["row"]
    col_devs = mesh.shape["col"]
    act_spec = P("ens", "row", "col", None)

    def local_stack(x_tile, weights, biases):
        batch, rows, cols, ch = x_tile.shape
        layers = weights.shape[0]
        imgs = batch // GROUPS
        halves = ch // LANES
        dims = (layers, imgs, rows, cols, ch, row_devs, col_devs)
        hbm = pl.BlockSpec(memory_space=pltpu.HBM)
        return pl.pallas_call(
            functools.partial(kernel, dims),
            out_shape=pltpu.VMEM((batch, rows, cols, ch), jnp.bfloat16),
            in_specs=[hbm, hbm, hbm],
            out_specs=pl.BlockSpec(memory_space=pltpu.VMEM),
            scratch_shapes=[
                pltpu.VMEM((layers * GROUPS, rows + 2, cols + 2, halves, imgs, LANES), jnp.bfloat16),
                pltpu.VMEM((layers, halves, TAPS * ch, LANES), jnp.bfloat16),
                pltpu.VMEM((layers, ch), jnp.float32),
                pltpu.VMEM((GROUPS, halves, imgs, rows, cols, LANES), jnp.bfloat16),
                pltpu.VMEM((imgs * imgs, imgs * imgs), jnp.bfloat16),
                pltpu.VMEM((GROUPS, rows, halves, imgs * (cols + 1), LANES), jnp.float32),
                pltpu.SemaphoreType.DMA(((GROUPS + layers) * halves + 1,)),
                pltpu.SemaphoreType.DMA((layers * GROUPS, len(NBRS))),
                pltpu.SemaphoreType.DMA((layers * GROUPS, len(NBRS))),
            ],
            compiler_params=pltpu.CompilerParams(collective_id=0, has_side_effects=True, vmem_limit_bytes=56 * 1024 * 1024),
            name="conv_stack",
        )(x_tile, weights.reshape(layers, TAPS * ch, ch), biases)

    return jax.shard_map(local_stack, mesh=mesh, in_specs=(act_spec, P(), P()), out_specs=act_spec, check_vma=False)
```

```python
import functools

import jax
import jax.numpy as jnp
from jax import lax
from jax.experimental import pallas as pl
from jax.experimental.pallas import tpu as pltpu
from jax.sharding import PartitionSpec as P

MESH = pl.DeviceIdType.MESH
LANES = 128
GROUPS = 2
TAPS = 9
NBRS = ((-1, 0), (1, 0), (0, -1), (0, 1), (-1, -1), (-1, 1), (1, -1), (1, 1))
SEND_ORDER = (4, 5, 6, 7, 2, 3, 0, 1)
EARLY_ROWS = 2


def row_taps(act, p, r, first, count):
    return [act[p, r + t // 3, pl.ds(first + t % 3, count)] for t in range(TAPS)]


def conv_dot(taps, w_vm, b_ref, layer, b_layer):
    halves = w_vm.shape[1]
    lhs = jnp.concatenate([tap[..., hf, :, :].reshape(-1, LANES) for tap in taps for hf in range(halves)], axis=1)
    wt = jnp.concatenate([w_vm[layer, hf] for hf in range(halves)], axis=1)
    y = jnp.dot(lhs, wt, preferred_element_type=jnp.float32)
    return jnp.maximum(y + b_ref[pl.ds(b_layer, 1), :], 0.0)


def keep_lines(lines, imgs, first, count, y):
    halves, length = lines.shape[:2]
    pitch = length // imgs
    for i in range(count):
        for hf in range(halves):
            lines[hf, pl.ds(first + i, imgs, stride=pitch), :] = y[i * imgs:(i + 1) * imgs, hf * LANES:(hf + 1) * LANES]


def write_lines(o_ref, lines, first_img, imgs, r):
    halves, length = lines.shape[:2]
    pitch, cols = length // imgs, o_ref.shape[2]
    for i in range(imgs):
        for hf in range(halves):
            line = lines[hf, pl.ds(i * pitch, cols), :].astype(jnp.bfloat16)
            o_ref[first_img + i, r, :, pl.ds(hf * LANES, LANES)] = line


def last_row(dims, done, act, w_vm, b_ref, o_hbm, lines, stage, sem):
    layers, imgs, rows, cols, ch = dims[:5]
    first_img = (GROUPS - 1) * imgs
    copies = []
    for g in range(GROUPS):
        count = rows if g < GROUPS - 1 else rows - 1
        where = (pl.ds(g * imgs, imgs), pl.ds(0, count))
        copies.append(pltpu.make_async_copy(done.at[where], o_hbm.at[where], sem.at[g]))
    for c in copies:
        c.start()
    half = cols // 2
    for first in (0, half):
        y = conv_dot(row_taps(act, 0, 0, first, half), w_vm, b_ref, 0, layers - 1)
        keep_lines(lines, imgs, first, half, y)
    write_lines(stage, lines, 0, imgs, 0)
    tail = pltpu.make_async_copy(stage, o_hbm.at[pl.ds(first_img, imgs), pl.ds(rows - 1, 1)], sem.at[GROUPS])
    tail.start()
    for c in copies + [tail]:
        c.wait()


def kernel(dims, x_hbm, w_hbm, b_hbm, o_ref, act_end, w_end, b_ref, act, w_vm, x_vm, perm, turn, in_sem, send_sem, recv_sem):
    layers, imgs, rows, cols, ch, row_devs, col_devs = dims
    halves = ch // LANES
    row, col = lax.axis_index("row"), lax.axis_index("col")

    has = {(-1, 0): row > 0, (1, 0): row < row_devs - 1, (0, -1): col > 0, (0, 1): col < col_devs - 1}

    def exists(dr, dc):
        if dr and dc:
            return jnp.logical_and(has[(dr, 0)], has[(0, dc)])
        return has[(dr, dc)]

    def span(step, size):
        if step < 0:
            return pl.ds(1, 1), pl.ds(size + 1, 1)
        if step > 0:
            return pl.ds(size, 1), pl.ds(0, 1)
        return pl.ds(1, size), pl.ds(1, size)

    def neighbour(n):
        return {"row": row + NBRS[n][0], "col": col + NBRS[n][1]}

    def edge_copy(buf, n):
        src_r, dst_r = span(NBRS[n][0], rows)
        src_c, dst_c = span(NBRS[n][1], cols)
        return pltpu.make_async_remote_copy(
            src_ref=act.at[buf, src_r, src_c],
            dst_ref=act.at[buf, dst_r, dst_c],
            send_sem=send_sem.at[buf, n],
            recv_sem=recv_sem.at[buf, n],
            device_id=neighbour(n),
            device_id_type=MESH,
        )

    def send(buf):
        for n in SEND_ORDER:
            @pl.when(exists(*NBRS[n]))
            def _(n=n):
                edge_copy(buf, n).start()

    def receive(buf):
        for n, (dr, dc) in enumerate(NBRS):
            @pl.when(exists(-dr, -dc))
            def _(n=n):
                edge_copy(buf, n).wait_recv()

    x_copies, w_copies = [], []
    for g in range(GROUPS):
        for hf in range(halves):
            x_copies.append(pltpu.make_async_copy(
                x_hbm.at[pl.ds(g * imgs, imgs), :, :, pl.ds(hf * LANES, LANES)], x_vm.at[g, hf], in_sem.at[g * halves + hf]))
    for l in range(layers):
        for hf in range(halves):
            w_copies.append(pltpu.make_async_copy(
                w_hbm.at[l, :, pl.ds(hf * LANES, LANES)], w_vm.at[l, hf], in_sem.at[(GROUPS + l) * halves + hf]))
    for hf in range(halves):
        w_copies.append(pltpu.make_async_copy(
            w_hbm.at[layers - 1, :, pl.ds(hf * LANES, LANES)], w_end.at[0, hf], in_sem.at[(GROUPS + layers) * halves + hf]))
    b_copy = pltpu.make_async_copy(b_hbm, b_ref, in_sem.at[(GROUPS + layers + 1) * halves])
    for c in x_copies[:halves] + w_copies[:halves] + [b_copy]:
        c.start()

    barrier = pltpu.get_barrier_semaphore()
    for n in range(len(NBRS)):
        @pl.when(exists(*NBRS[n]))
        def _(n=n):
            pl.semaphore_signal(barrier, inc=1, device_id=neighbour(n), device_id_type=MESH)

    def zero_borders(buf, carry):
        @pl.when(row == 0)
        def _():
            act[buf, 0] = jnp.zeros(act.shape[2:], act.dtype)

        @pl.when(row == row_devs - 1)
        def _():
            act[buf, rows + 1] = jnp.zeros(act.shape[2:], act.dtype)

        @pl.when(col == 0)
        def _():
            act[buf, pl.ds(0, rows + 2), 0] = jnp.zeros((rows + 2,) + act.shape[3:], act.dtype)

        @pl.when(col == col_devs - 1)
        def _():
            act[buf, pl.ds(0, rows + 2), cols + 1] = jnp.zeros((rows + 2,) + act.shape[3:], act.dtype)
        return carry

    lax.fori_loop(0, layers * GROUPS, zero_borders, 0)

    block = imgs * imgs
    out_row = lax.broadcasted_iota(jnp.int32, (block, block), 0)
    in_row = lax.broadcasted_iota(jnp.int32, (block, block), 1)
    swapped = (out_row % imgs) * imgs + out_row // imgs
    perm[...] = jnp.where(in_row == swapped, 1.0, 0.0).astype(jnp.bfloat16)

    for c in x_copies[halves:]:
        c.start()

    def put(buf, r, first, count, y):
        for hf in range(halves):
            act[buf, r + 1, pl.ds(first + 1, count), hf] = y[:, hf * LANES:(hf + 1) * LANES].reshape(count, imgs, LANES)

    order = (0, rows - 1) + tuple(range(1, rows - 1))

    def turn_input(g):
        for hf in range(halves):
            x_copies[g * halves + hf].wait()
        for r in order:
            for first in range(0, cols, imgs):
                tile = jnp.concatenate([x_vm[g, hf, :, r, pl.ds(first, imgs)].reshape(block, LANES) for hf in range(halves)], axis=1)
                y = jnp.dot(perm[...], tile, preferred_element_type=jnp.float32)
                put(g, r, first, imgs, y.astype(jnp.bfloat16))

    def conv(taps, layer):
        return conv_dot(taps, w_vm, b_ref, layer, layer)

    def conv_row(p, layer, r, first, count):
        return conv(row_taps(act, p, r, first, count), layer)

    def keep(buf, r, first, count, y):
        put(buf, r, first, count, y.astype(jnp.bfloat16))

    def keep_last(buf, r, first, count, y):
        keep_lines(turn.at[buf - layers * GROUPS, r], imgs, first, count, y)

    def write_row(g, r):
        write_lines(o_ref, turn.at[g, r], g * imgs, imgs, r)

    def interior(p, which, store):
        for r in which:
            store(p + GROUPS, r, 1, cols - 2, conv_row(p, p // GROUPS, r, 1, cols - 2))

    def side_taps(p, c):
        return [act[p, pl.ds(1 + t // 3, rows - 2), c + t % 3] for t in range(TAPS)]

    inner = range(1, rows - 1)
    corners = ((0, 0), (rows - 1, cols - 1))

    def edges(p):
        edge = cols * imgs
        for r, c in corners:
            side = side_taps(p, c)
            taps = [jnp.concatenate([act[p, r + t // 3, pl.ds(t % 3, cols)], side[t]], axis=0) for t in range(TAPS)]
            y = conv(taps, p // GROUPS).astype(jnp.bfloat16)
            put(p + GROUPS, r, 0, cols, y[:edge])
            for hf in range(halves):
                act[p + GROUPS, pl.ds(2, rows - 2), c + 1, hf] = y[edge:, hf * LANES:(hf + 1) * LANES].reshape(rows - 2, imgs, LANES)

    turn_input(0)
    for c in w_copies[:halves] + [b_copy]:
        c.wait()
    turn_input(1)
    interior(0, inner[:EARLY_ROWS], keep)
    n_row = 1 + sum(has[(d, 0)].astype(jnp.int32) for d in (-1, 1))
    n_col = 1 + sum(has[(0, d)].astype(jnp.int32) for d in (-1, 1))
    pl.semaphore_wait(barrier, n_row * n_col - 1)
    for g in range(GROUPS):
        send(g)
    for c in w_copies[halves:]:
        c.start()
    interior(0, inner[EARLY_ROWS:], keep)
    interior(1, inner, keep)
    for c in w_copies[halves:]:
        c.wait()

    def middle(p, carry):
        receive(p)
        edges(p)
        send(p + GROUPS)
        interior(p + GROUPS, inner, keep)
        return carry

    lax.fori_loop(0, (layers - 2) * GROUPS, middle, 0)

    def next_to_last(p, carry):
        receive(p)
        edges(p)
        send(p + GROUPS)
        interior(p + GROUPS, inner, keep_last)
        return carry

    lax.fori_loop((layers - 2) * GROUPS, (layers - 1) * GROUPS, next_to_last, 0)

    def sides(p):
        receive(p)
        for _, c in corners:
            y = conv(side_taps(p, c), layers - 1)
            for i in range(rows - 2):
                keep_last(p + GROUPS, i + 1, c, 1, y[i * imgs:(i + 1) * imgs])

    end = layers * GROUPS
    for p in range(end - GROUPS, end - 1):
        g = p - (end - GROUPS)
        sides(p)
        for r, _ in corners:
            keep_last(p + GROUPS, r, 0, cols, conv_row(p, layers - 1, r, 0, cols))
            if r == 0:
                for i in inner:
                    write_row(g, i)
    sides(end - 1)
    for r, _ in corners:
        write_row(0, r)
    act_end[0] = act[end - 1, pl.ds(rows - 1, 3)]
    half = cols // 2
    for first in (0, half):
        keep_last(end - 1 + GROUPS, 0, first, half, conv_row(end - 1, layers - 1, 0, first, half))
    for i in inner:
        write_row(GROUPS - 1, i)
    write_row(GROUPS - 1, 0)

    def finish(buf, carry):
        for n in range(len(NBRS)):
            @pl.when(exists(*NBRS[n]))
            def _(n=n):
                edge_copy(buf, n).wait_send()
        return carry

    lax.fori_loop(0, layers * GROUPS, finish, 0)


def solution(mesh):
    row_devs = mesh.shape["row"]
    col_devs = mesh.shape["col"]
    act_spec = P("ens", "row", "col", None)

    def local_stack(x_tile, weights, biases):
        batch, rows, cols, ch = x_tile.shape
        layers = weights.shape[0]
        imgs = batch // GROUPS
        halves = ch // LANES
        dims = (layers, imgs, rows, cols, ch, row_devs, col_devs)
        hbm = pl.BlockSpec(memory_space=pltpu.HBM)
        vmem = pl.BlockSpec(memory_space=pltpu.VMEM)
        pitch = cols + 1
        done, act_end, w_end, b_vm = pl.pallas_call(
            functools.partial(kernel, dims),
            out_shape=[
                pltpu.VMEM((batch, rows, cols, ch), jnp.bfloat16),
                pltpu.VMEM((1, 3, cols + 2, halves, imgs, LANES), jnp.bfloat16),
                pltpu.VMEM((1, halves, TAPS * ch, LANES), jnp.bfloat16),
                pltpu.VMEM((layers, ch), jnp.float32),
            ],
            in_specs=[hbm, hbm, hbm],
            out_specs=[vmem] * 4,
            scratch_shapes=[
                pltpu.VMEM((layers * GROUPS, rows + 2, cols + 2, halves, imgs, LANES), jnp.bfloat16),
                pltpu.VMEM((layers, halves, TAPS * ch, LANES), jnp.bfloat16),
                pltpu.VMEM((GROUPS, halves, imgs, rows, cols, LANES), jnp.bfloat16),
                pltpu.VMEM((imgs * imgs, imgs * imgs), jnp.bfloat16),
                pltpu.VMEM((GROUPS, rows, halves, imgs * pitch, LANES), jnp.float32),
                pltpu.SemaphoreType.DMA(((GROUPS + layers + 1) * halves + 1,)),
                pltpu.SemaphoreType.DMA((layers * GROUPS, len(NBRS))),
                pltpu.SemaphoreType.DMA((layers * GROUPS, len(NBRS))),
            ],
            compiler_params=pltpu.CompilerParams(collective_id=0, has_side_effects=True, vmem_limit_bytes=55 * 1024 * 1024),
            name="conv_stack",
        )(x_tile, weights.reshape(layers, TAPS * ch, ch), biases)
        return pl.pallas_call(
            functools.partial(last_row, dims),
            out_shape=jax.ShapeDtypeStruct((batch, rows, cols, ch), jnp.bfloat16),
            in_specs=[vmem] * 4,
            out_specs=hbm,
            scratch_shapes=[
                pltpu.VMEM((halves, imgs * pitch, LANES), jnp.float32),
                pltpu.VMEM((imgs, 1, cols, ch), jnp.bfloat16),
                pltpu.SemaphoreType.DMA((GROUPS + 1,)),
            ],
            compiler_params=pltpu.CompilerParams(vmem_limit_bytes=16 * 1024 * 1024),
            name="last_row",
        )(done, act_end, w_end, b_vm)

    return jax.shard_map(local_stack, mesh=mesh, in_specs=(act_spec, P(), P()), out_specs=act_spec, check_vma=False)
```

```python
import functools

import jax
import jax.numpy as jnp
from jax import lax
from jax.experimental import pallas as pl
from jax.experimental.pallas import tpu as pltpu
from jax.sharding import PartitionSpec as P

MESH = pl.DeviceIdType.MESH
LANES = 128
GROUPS = 2
TAPS = 9
NBRS = ((-1, 0), (1, 0), (0, -1), (0, 1), (-1, -1), (-1, 1), (1, -1), (1, 1))
SEND_ORDER = (4, 5, 6, 7, 2, 3, 0, 1)


def row_taps(act, p, r, first, count):
    return [act[p, r + t // 3, pl.ds(first + t % 3, count)] for t in range(TAPS)]


def conv_dot(taps, w_vm, b_ref, layer, b_layer):
    halves = w_vm.shape[1]
    lhs = jnp.concatenate([tap[..., hf, :, :].reshape(-1, LANES) for tap in taps for hf in range(halves)], axis=1)
    wt = jnp.concatenate([w_vm[layer, hf] for hf in range(halves)], axis=1)
    y = jnp.dot(lhs, wt, preferred_element_type=jnp.float32)
    return jnp.maximum(y + b_ref[pl.ds(b_layer, 1), :], 0.0)


def keep_lines(lines, imgs, first, count, y):
    halves, length = lines.shape[:2]
    pitch = length // imgs
    for i in range(count):
        for hf in range(halves):
            lines[hf, pl.ds(first + i, imgs, stride=pitch), :] = y[i * imgs:(i + 1) * imgs, hf * LANES:(hf + 1) * LANES]


def write_lines(o_ref, lines, first_img, imgs, r):
    halves, length = lines.shape[:2]
    pitch, cols = length // imgs, o_ref.shape[2]
    for i in range(imgs):
        for hf in range(halves):
            line = lines[hf, pl.ds(i * pitch, cols), :].astype(jnp.bfloat16)
            o_ref[first_img + i, r, :, pl.ds(hf * LANES, LANES)] = line


def last_row(dims, done, act, w_vm, b_ref, o_hbm, lines, stage, sem):
    layers, imgs, rows, cols, ch = dims[:5]
    first_img = (GROUPS - 1) * imgs
    copies = []
    for g in range(GROUPS):
        count = rows if g < GROUPS - 1 else rows - 1
        where = (pl.ds(g * imgs, imgs), pl.ds(0, count))
        copies.append(pltpu.make_async_copy(done.at[where], o_hbm.at[where], sem.at[g]))
    for c in copies:
        c.start()
    half = cols // 2
    for first in (0, half):
        y = conv_dot(row_taps(act, 0, 0, first, half), w_vm, b_ref, 0, layers - 1)
        keep_lines(lines, imgs, first, half, y)
    write_lines(stage, lines, 0, imgs, 0)
    tail = pltpu.make_async_copy(stage, o_hbm.at[pl.ds(first_img, imgs), pl.ds(rows - 1, 1)], sem.at[GROUPS])
    tail.start()
    for c in copies + [tail]:
        c.wait()


def kernel(dims, x_hbm, w_hbm, b_hbm, o_ref, act_end, w_end, b_ref, act, w_vm, x_vm, perm, turn, in_sem, send_sem, recv_sem):
    layers, imgs, rows, cols, ch, row_devs, col_devs = dims
    halves = ch // LANES
    row, col = lax.axis_index("row"), lax.axis_index("col")

    has = {(-1, 0): row > 0, (1, 0): row < row_devs - 1, (0, -1): col > 0, (0, 1): col < col_devs - 1}

    def exists(dr, dc):
        if dr and dc:
            return jnp.logical_and(has[(dr, 0)], has[(0, dc)])
        return has[(dr, dc)]

    def span(step, size):
        if step < 0:
            return pl.ds(1, 1), pl.ds(size + 1, 1)
        if step > 0:
            return pl.ds(size, 1), pl.ds(0, 1)
        return pl.ds(1, size), pl.ds(1, size)

    def neighbour(n):
        return {"row": row + NBRS[n][0], "col": col + NBRS[n][1]}

    def edge_copy(buf, n):
        src_r, dst_r = span(NBRS[n][0], rows)
        src_c, dst_c = span(NBRS[n][1], cols)
        return pltpu.make_async_remote_copy(
            src_ref=act.at[buf, src_r, src_c],
            dst_ref=act.at[buf, dst_r, dst_c],
            send_sem=send_sem.at[buf, n],
            recv_sem=recv_sem.at[buf, n],
            device_id=neighbour(n),
            device_id_type=MESH,
        )

    def send(buf):
        for n in SEND_ORDER:
            @pl.when(exists(*NBRS[n]))
            def _(n=n):
                edge_copy(buf, n).start()

    def receive(buf):
        for n, (dr, dc) in enumerate(NBRS):
            @pl.when(exists(-dr, -dc))
            def _(n=n):
                edge_copy(buf, n).wait_recv()

    x_copies, w_copies = [], []
    for g in range(GROUPS):
        for hf in range(halves):
            x_copies.append(pltpu.make_async_copy(
                x_hbm.at[pl.ds(g * imgs, imgs), :, :, pl.ds(hf * LANES, LANES)], x_vm.at[g, hf], in_sem.at[g * halves + hf]))
    for l in range(layers):
        for hf in range(halves):
            w_copies.append(pltpu.make_async_copy(
                w_hbm.at[l, :, pl.ds(hf * LANES, LANES)], w_vm.at[l, hf], in_sem.at[(GROUPS + l) * halves + hf]))
    for hf in range(halves):
        w_copies.append(pltpu.make_async_copy(
            w_hbm.at[layers - 1, :, pl.ds(hf * LANES, LANES)], w_end.at[0, hf], in_sem.at[(GROUPS + layers) * halves + hf]))
    b_copy = pltpu.make_async_copy(b_hbm, b_ref, in_sem.at[(GROUPS + layers + 1) * halves])
    for c in x_copies:
        c.start()

    barrier = pltpu.get_barrier_semaphore()
    for n in range(len(NBRS)):
        @pl.when(exists(*NBRS[n]))
        def _(n=n):
            pl.semaphore_signal(barrier, inc=1, device_id=neighbour(n), device_id_type=MESH)

    def zero_borders(buf, carry):
        @pl.when(row == 0)
        def _():
            act[buf, 0] = jnp.zeros(act.shape[2:], act.dtype)

        @pl.when(row == row_devs - 1)
        def _():
            act[buf, rows + 1] = jnp.zeros(act.shape[2:], act.dtype)

        @pl.when(col == 0)
        def _():
            act[buf, pl.ds(0, rows + 2), 0] = jnp.zeros((rows + 2,) + act.shape[3:], act.dtype)

        @pl.when(col == col_devs - 1)
        def _():
            act[buf, pl.ds(0, rows + 2), cols + 1] = jnp.zeros((rows + 2,) + act.shape[3:], act.dtype)
        return carry

    lax.fori_loop(0, layers * GROUPS, zero_borders, 0)

    block = imgs * imgs
    out_row = lax.broadcasted_iota(jnp.int32, (block, block), 0)
    in_row = lax.broadcasted_iota(jnp.int32, (block, block), 1)
    swapped = (out_row % imgs) * imgs + out_row // imgs
    perm[...] = jnp.where(in_row == swapped, 1.0, 0.0).astype(jnp.bfloat16)

    for c in w_copies[:halves] + [b_copy]:
        c.start()

    def put(buf, r, first, count, y):
        for hf in range(halves):
            act[buf, r + 1, pl.ds(first + 1, count), hf] = y[:, hf * LANES:(hf + 1) * LANES].reshape(count, imgs, LANES)

    order = (0, rows - 1) + tuple(range(1, rows - 1))

    def turn_input(g):
        for hf in range(halves):
            x_copies[g * halves + hf].wait()
        for r in order:
            for first in range(0, cols, imgs):
                tile = jnp.concatenate([x_vm[g, hf, :, r, pl.ds(first, imgs)].reshape(block, LANES) for hf in range(halves)], axis=1)
                y = jnp.dot(perm[...], tile, preferred_element_type=jnp.float32)
                put(g, r, first, imgs, y.astype(jnp.bfloat16))

    def conv(taps, layer):
        return conv_dot(taps, w_vm, b_ref, layer, layer)

    def conv_row(p, layer, r, first, count):
        return conv(row_taps(act, p, r, first, count), layer)

    def keep(buf, r, first, count, y):
        put(buf, r, first, count, y.astype(jnp.bfloat16))

    def keep_last(buf, r, first, count, y):
        keep_lines(turn.at[buf - layers * GROUPS, r], imgs, first, count, y)

    def write_row(g, r):
        write_lines(o_ref, turn.at[g, r], g * imgs, imgs, r)

    def interior(p, which, store):
        for r in which:
            store(p + GROUPS, r, 1, cols - 2, conv_row(p, p // GROUPS, r, 1, cols - 2))

    def side_taps(p, c):
        return [act[p, pl.ds(1 + t // 3, rows - 2), c + t % 3] for t in range(TAPS)]

    inner = range(1, rows - 1)
    corners = ((0, 0), (rows - 1, cols - 1))

    def edges(p):
        edge = cols * imgs
        for r, c in corners:
            side = side_taps(p, c)
            taps = [jnp.concatenate([act[p, r + t // 3, pl.ds(t % 3, cols)], side[t]], axis=0) for t in range(TAPS)]
            y = conv(taps, p // GROUPS).astype(jnp.bfloat16)
            put(p + GROUPS, r, 0, cols, y[:edge])
            for hf in range(halves):
                act[p + GROUPS, pl.ds(2, rows - 2), c + 1, hf] = y[edge:, hf * LANES:(hf + 1) * LANES].reshape(rows - 2, imgs, LANES)

    turn_input(0)
    turn_input(1)
    for c in w_copies[:halves] + [b_copy]:
        c.wait()
    n_row = 1 + sum(has[(d, 0)].astype(jnp.int32) for d in (-1, 1))
    n_col = 1 + sum(has[(0, d)].astype(jnp.int32) for d in (-1, 1))
    pl.semaphore_wait(barrier, n_row * n_col - 1)
    for g in range(GROUPS):
        send(g)
    for c in w_copies[halves:]:
        c.start()
    interior(0, inner, keep)
    interior(1, inner, keep)
    for c in w_copies[halves:]:
        c.wait()

    def middle(p, carry):
        receive(p)
        edges(p)
        send(p + GROUPS)
        interior(p + GROUPS, inner, keep)
        return carry

    lax.fori_loop(0, (layers - 2) * GROUPS, middle, 0)

    def next_to_last(p, carry):
        receive(p)
        edges(p)
        send(p + GROUPS)
        interior(p + GROUPS, inner, keep_last)
        return carry

    lax.fori_loop((layers - 2) * GROUPS, (layers - 1) * GROUPS, next_to_last, 0)

    def sides(p):
        receive(p)
        for _, c in corners:
            y = conv(side_taps(p, c), layers - 1)
            for i in range(rows - 2):
                keep_last(p + GROUPS, i + 1, c, 1, y[i * imgs:(i + 1) * imgs])

    end = layers * GROUPS
    for p in range(end - GROUPS, end - 1):
        g = p - (end - GROUPS)
        sides(p)
        for r, _ in corners:
            keep_last(p + GROUPS, r, 0, cols, conv_row(p, layers - 1, r, 0, cols))
            if r == 0:
                for i in inner:
                    write_row(g, i)
    sides(end - 1)
    for r, _ in corners:
        write_row(0, r)
    act_end[0] = act[end - 1, pl.ds(rows - 1, 3)]
    half = cols // 2
    for first in (0, half):
        keep_last(end - 1 + GROUPS, 0, first, half, conv_row(end - 1, layers - 1, 0, first, half))
    for i in inner:
        write_row(GROUPS - 1, i)
    write_row(GROUPS - 1, 0)

    def finish(buf, carry):
        for n in range(len(NBRS)):
            @pl.when(exists(*NBRS[n]))
            def _(n=n):
                edge_copy(buf, n).wait_send()
        return carry

    lax.fori_loop(0, layers * GROUPS, finish, 0)


def solution(mesh):
    row_devs = mesh.shape["row"]
    col_devs = mesh.shape["col"]
    act_spec = P("ens", "row", "col", None)

    def local_stack(x_tile, weights, biases):
        batch, rows, cols, ch = x_tile.shape
        layers = weights.shape[0]
        imgs = batch // GROUPS
        halves = ch // LANES
        dims = (layers, imgs, rows, cols, ch, row_devs, col_devs)
        hbm = pl.BlockSpec(memory_space=pltpu.HBM)
        vmem = pl.BlockSpec(memory_space=pltpu.VMEM)
        pitch = cols + 1
        done, act_end, w_end, b_vm = pl.pallas_call(
            functools.partial(kernel, dims),
            out_shape=[
                pltpu.VMEM((batch, rows, cols, ch), jnp.bfloat16),
                pltpu.VMEM((1, 3, cols + 2, halves, imgs, LANES), jnp.bfloat16),
                pltpu.VMEM((1, halves, TAPS * ch, LANES), jnp.bfloat16),
                pltpu.VMEM((layers, ch), jnp.float32),
            ],
            in_specs=[hbm, hbm, hbm],
            out_specs=[vmem] * 4,
            scratch_shapes=[
                pltpu.VMEM((layers * GROUPS, rows + 2, cols + 2, halves, imgs, LANES), jnp.bfloat16),
                pltpu.VMEM((layers, halves, TAPS * ch, LANES), jnp.bfloat16),
                pltpu.VMEM((GROUPS, halves, imgs, rows, cols, LANES), jnp.bfloat16),
                pltpu.VMEM((imgs * imgs, imgs * imgs), jnp.bfloat16),
                pltpu.VMEM((GROUPS, rows, halves, imgs * pitch, LANES), jnp.float32),
                pltpu.SemaphoreType.DMA(((GROUPS + layers + 1) * halves + 1,)),
                pltpu.SemaphoreType.DMA((layers * GROUPS, len(NBRS))),
                pltpu.SemaphoreType.DMA((layers * GROUPS, len(NBRS))),
            ],
            compiler_params=pltpu.CompilerParams(collective_id=0, has_side_effects=True, vmem_limit_bytes=55 * 1024 * 1024),
            name="conv_stack",
        )(x_tile, weights.reshape(layers, TAPS * ch, ch), biases)
        return pl.pallas_call(
            functools.partial(last_row, dims),
            out_shape=jax.ShapeDtypeStruct((batch, rows, cols, ch), jnp.bfloat16),
            in_specs=[vmem] * 4,
            out_specs=hbm,
            scratch_shapes=[
                pltpu.VMEM((halves, imgs * pitch, LANES), jnp.float32),
                pltpu.VMEM((imgs, 1, cols, ch), jnp.bfloat16),
                pltpu.SemaphoreType.DMA((GROUPS + 1,)),
            ],
            compiler_params=pltpu.CompilerParams(vmem_limit_bytes=16 * 1024 * 1024),
            name="last_row",
        )(done, act_end, w_end, b_vm)

    return jax.shard_map(local_stack, mesh=mesh, in_specs=(act_spec, P(), P()), out_specs=act_spec, check_vma=False)
```
